32 devices in a mesh: lat: 4 (over x, core), lon: 8 (over z, y).
Axes of the slice: x: 2, y: 2, z: 4, core: 2. Of those that a mesh axis runs over, the one named last changes fastest.
Arguments:
- prediction_fields: float32 [4, 69, 360, 512], P(None, None, 'lon', 'lat'), may hold values from -16 to 16
- verifying_state: float32 [69, 360, 512], P(None, 'lon', 'lat'), may hold values from -16 to 16
- normal_state: float32 [69, 360, 512], P(None, 'lon', 'lat'), may hold values from -16 to 16
- evaluated_point_flag: int32 [360, 512], P('lon', 'lat'), may hold values 0 or 1
- parallels_each_strip: int32 [4], replicated, may hold values from 1 to 128, 361 in all
Outputs:
- parallel_quadratic_error: float32 [4, 69, 512], P(None, None, 'lat')
- parallel_systematic_error: float32 [4, 69, 512], P(None, None, 'lat')
- parallel_pattern_skill: float32 [4, 69, 512], P(None, None, 'lat')
- rmse: float32 [4, 69], replicated
- systematic_error: float32 [4, 69], replicated
- pattern_skill: float32 [4, 69], replicated
The draws below stay inside these ranges and needn't reach their ends.
Inputs may be any that keep to these rules, and one draw needn't show every extreme that they name: `parallels_each_strip`: they sum to 361, and some band holds exactly 128 rows.
All inputs are finite; a program needn't handle non-finite values.
Results may differ from the reference program's by a relative error of at most 0.00002.
Values sent between devices are 32-bit elements.
A program may use at most 64 MiB of HBM per device.

```python
import math
import jax
import jax.numpy as jnp
import numpy as np
from jax import lax

VARS = 69
LEADS = 4
LAT_CAP = 128
LAT_BANDS = 4
NLAT = 361
EAST_WEST_SIZE = 360
LAT_BUF = 512


def common_fields(key):
    subkeys = jax.random.split(jax.random.fold_in(key, 4242), 8)
    climate = jax.random.normal(subkeys[0], (VARS, EAST_WEST_SIZE, LAT_BUF), jnp.float32)
    amplitude = jnp.exp(jax.random.uniform(subkeys[1], (VARS, 1, LAT_BUF), jnp.float32, jnp.log(0.5), jnp.log(2.0)))
    anomaly = jax.random.normal(subkeys[2], (VARS, EAST_WEST_SIZE, LAT_BUF), jnp.float32) * amplitude
    observed = climate + anomaly
    skill = jax.random.uniform(subkeys[4], (LEADS, VARS, 1, 1), jnp.float32, 0.3, 0.95)
    noise_scale = jax.random.uniform(subkeys[5], (LEADS, VARS, 1, 1), jnp.float32, 0.6, 1.2)
    drift = jax.random.uniform(subkeys[6], (LEADS, VARS, 1, LAT_BUF), jnp.float32, -0.6, 0.6)
    noise = jax.random.normal(subkeys[7], (LEADS, VARS, EAST_WEST_SIZE, LAT_BUF), jnp.float32)
    predicted = climate[None] + skill * anomaly[None] + noise_scale * amplitude[None] * noise + drift
    return (jnp.clip(predicted, -16.0, 16.0), jnp.clip(observed, -16.0, 16.0), jnp.clip(climate, -16.0, 16.0))


def draw_prediction_fields(key, part):
    return common_fields(key)[0]


def draw_verifying_state(key, part):
    return common_fields(key)[1]


def draw_normal_state(key, part):
    return common_fields(key)[2]


def place_ends(values, own_key, least, top_value):
    extent = values.shape
    index_at = [jax.random.randint(jax.random.fold_in(own_key, axis), (), 0, extent[axis]) for axis in range(len(extent))]
    values = values.at[tuple(index_at)].set(least)
    longest = extent.index(max(extent))
    index_at[longest] = (index_at[longest] + 1) % extent[longest]
    return values.at[tuple(index_at)].set(top_value)


def length_profile(count, total, limit, skew):
    portions = [(1 << 20) // math.isqrt(grade ** skew) + 1 for grade in range(2, count + 1)]
    spare, given = total - limit - (count - 1), [1] * (count - 1)
    while spare > 0:
        free = [i for i in range(count - 1) if given[i] < limit]
        mass, remaining = sum([portions[i] for i in free]), spare
        for i in free:
            extra = min(limit - given[i], max(1, remaining * portions[i] // mass), spare)
            given[i] = given[i] + extra
            spare = spare - extra
    return np.array([limit] + given)


def ragged(own_key, number_of, total, most, slope):
    if number_of == 2:
        one = jax.random.randint(own_key, (), max(1, total - most), min(most, total - 1) + 1)
        return jnp.stack([one, total - one])
    sizes = jnp.asarray(length_profile(number_of, total, most, slope), jnp.int32)
    twos = (number_of - 1) // 2
    donor, taker = sizes[1:1 + 2 * twos:2], sizes[2:2 + 2 * twos:2]
    margin = jnp.minimum(donor - 1, most - taker)
    passed = jax.random.randint(jax.random.fold_in(own_key, 1), (twos,), 0, 1 << 20) % (margin + 1)
    sizes = sizes.at[1:1 + 2 * twos:2].set(donor - passed).at[2:2 + 2 * twos:2].set(taker + passed)
    return sizes[jax.random.permutation(jax.random.fold_in(own_key, 2), number_of)]


def setup_inputs(seed: int = 0) -> dict:
    arg_keys = jax.random.split(jax.random.key(seed), 6)
    return {
        "prediction_fields": draw_prediction_fields(jax.random.fold_in(arg_keys[5], 71), 0),
        "verifying_state": draw_verifying_state(jax.random.fold_in(arg_keys[5], 71), 0),
        "normal_state": draw_normal_state(jax.random.fold_in(arg_keys[5], 71), 0),
        "evaluated_point_flag": place_ends((jax.random.randint(arg_keys[3], (EAST_WEST_SIZE, LAT_BUF), 0, 4) < 3).astype(jnp.int32), jax.random.fold_in(arg_keys[3], 1), 0, 1),
        "parallels_each_strip": ragged(arg_keys[4], LAT_BANDS, NLAT, LAT_CAP, 2).astype(jnp.int32),
    }


minimum_divisor = 0.1

def final_result(error_power_two, prediction_error, paired_anomaly_term, predicted_spread_sum, observed_dispersion, grid_point_tally):
    mean_square = error_power_two / grid_point_tally
    average_error = prediction_error / grid_point_tally
    covariance_sum = paired_anomaly_term / grid_point_tally / jnp.sqrt(jnp.maximum(predicted_spread_sum / grid_point_tally, minimum_divisor) * jnp.maximum(observed_dispersion / grid_point_tally, minimum_divisor))
    return (mean_square, average_error, covariance_sum)

def reference(prediction_fields, verifying_state, normal_state, evaluated_point_flag, parallels_each_strip):
    band_start = jnp.cumsum(parallels_each_strip) - parallels_each_strip
    slot_ids = jnp.arange(LAT_CAP, dtype=jnp.int32)
    global_row = (band_start[:, None] + slot_ids[None, :]).reshape(-1)
    inside_band = (slot_ids[None, :] < parallels_each_strip[:, None]).reshape(-1)
    angles = jnp.pi * jnp.arange(NLAT, dtype=jnp.float32) / (NLAT - 1)
    normalizer = jnp.sum(jnp.sin(angles))
    row_angle = jnp.pi * global_row.astype(jnp.float32) / (NLAT - 1)
    area_factors = jnp.where(inside_band, jnp.sin(row_angle) * NLAT / normalizer, 0.0).astype(jnp.float32)
    retain_filter = evaluated_point_flag.astype(jnp.float32) * inside_band.astype(jnp.float32)[None, :]
    observed_anomaly = verifying_state - normal_state
    observed_dispersion = lax.optimization_barrier(jnp.sum(retain_filter * observed_anomaly * observed_anomaly, axis=1))

    def by_horizon(predicted_step):
        predicted_anomaly = predicted_step - normal_state
        mistake_field = predicted_anomaly - observed_anomaly
        return (lax.optimization_barrier(jnp.sum(retain_filter * mistake_field * mistake_field, axis=1)), lax.optimization_barrier(jnp.sum(retain_filter * mistake_field, axis=1)), lax.optimization_barrier(jnp.sum(retain_filter * predicted_anomaly * observed_anomaly, axis=1)), lax.optimization_barrier(jnp.sum(retain_filter * predicted_anomaly * predicted_anomaly, axis=1)))
    error_power_two, prediction_error, paired_anomaly_term, predicted_spread_sum = lax.map(by_horizon, prediction_fields)
    parallel_quadratic_error, parallel_systematic_error, parallel_pattern_skill = final_result(error_power_two, prediction_error, paired_anomaly_term, predicted_spread_sum, observed_dispersion[None], EAST_WEST_SIZE)
    grid_points = NLAT * EAST_WEST_SIZE
    quadratic_error_total, systematic_error, pattern_skill = final_result(lax.optimization_barrier(jnp.sum(error_power_two * area_factors, axis=-1)), lax.optimization_barrier(jnp.sum(prediction_error * area_factors, axis=-1)), lax.optimization_barrier(jnp.sum(paired_anomaly_term * area_factors, axis=-1)), lax.optimization_barrier(jnp.sum(predicted_spread_sum * area_factors, axis=-1)), lax.optimization_barrier(jnp.sum(observed_dispersion * area_factors, axis=-1))[None], grid_points)
    rmse = jnp.sqrt(jnp.maximum(quadratic_error_total, minimum_divisor))
    return (parallel_quadratic_error, parallel_systematic_error, parallel_pattern_skill, rmse, systematic_error, pattern_skill)
```

```python
import functools
import math

import jax
import jax.numpy as jnp
from jax import lax
from jax.experimental import pallas as pl
from jax.experimental.pallas import tpu as pltpu
from jax.sharding import PartitionSpec as P

MEAN_ROWS = 90
FLOOR = 0.1
LIMIT = 58 << 20
MESH = pl.DeviceIdType.MESH


def cosine(y):
    y2 = y * y
    terms = [(-1) ** k / math.factorial(2 * k) for k in range(9)]
    total = jnp.full_like(y, terms[-1])
    for term in terms[-2::-1]:
        total = total * y2 + term
    return total


def kernel(n_lat, n_lon, vp, par, pred, ver, norm, flag, o_sq, o_off, o_skill, g_rmse, g_off, g_skill,
           xp, xv, xn, xf, kf, spread_t, part, one_in, two_out, two_in, tot, flat, fin, g_out, g_in, g_mine, g_all, g_tmp,
           in_sem, pred_sem, one_s, one_r, two_s, two_r, agz_s, agz_r, agy_s, agy_r, lat_s, lat_r, lon_s, lon_r):
    nvars, cols, leads, lanes = pred.shape
    pair = 2 if n_lon % 2 == 0 else 1
    outer = n_lon // pair
    band = lax.axis_index("lat")
    me = lax.axis_index("lon")
    a, b = me // pair, me % pair
    ob = (pair - 1) - b
    lv = leads * vp
    blocks = part.shape[1]

    starts = [min(d * vp, nvars - vp) for d in range(n_lon)]

    def first_var(d):
        return jnp.minimum(d * vp, nvars - vp)

    def other(k):
        return lax.rem(a + k, outer)

    steps = [k for k in range(1, outer)] + [0]
    order = [(k, True) for k in steps] if pair == 2 else []
    order += [(k, False) for k in steps]
    first = [
        pltpu.make_async_copy(flag, xf, in_sem.at[0]),
        pltpu.make_async_copy(norm, xn, in_sem.at[1]),
        pltpu.make_async_copy(ver, xv, in_sem.at[2]),
    ]
    for c in first:
        c.start()
    chunk_vars, copies = [], []
    for i, (k, away) in enumerate(order):
        v0 = first_var(other(k) * pair + (ob if away else b))
        c = pltpu.make_async_copy(pred.at[pl.ds(v0, vp)], xp.at[i], pred_sem.at[i])
        c.start()
        chunk_vars.append(v0)
        copies.append(c)

    barrier = pltpu.get_barrier_semaphore()
    for k in range(1, n_lon):
        pl.semaphore_signal(barrier, inc=1, device_id=(band, lax.rem(me + k, n_lon)), device_id_type=MESH)
    for k in range(1, n_lat):
        pl.semaphore_signal(barrier, inc=1, device_id=(lax.rem(band + k, n_lat), me), device_id_type=MESH)

    first_row = jnp.int32(0)
    filled = jnp.int32(0)
    for i in range(n_lat):
        first_row = first_row + jnp.where(i < band, par[i], 0)
        filled = filled + jnp.where(i == band, par[i], 0)
    total_rows = MEAN_ROWS * n_lat + 1
    slot = lax.broadcasted_iota(jnp.int32, (8, lanes), 1)
    g = (first_row + slot).astype(jnp.float32)
    normalizer = sum(math.sin(math.pi * r / (total_rows - 1)) for r in range(total_rows))
    angle = (g - 0.5 * (total_rows - 1)) * (math.pi / (total_rows - 1))
    weight = jnp.where(slot < filled, cosine(angle) * (total_rows / normalizer), 0.0)
    if vp % 4:
        for i in range(n_lon):
            part[i, blocks - 1] = jnp.zeros((4, lanes), jnp.float32)

    first[0].wait()
    kf[...] = jnp.where(lax.broadcasted_iota(jnp.int32, (cols, lanes), 1) < filled, xf[...].astype(jnp.float32), 0.0)
    first[1].wait()
    first[2].wait()

    def truth_column(c, total):
        t = kf[pl.ds(c, 1), :] * (xv[c] - xn[c])
        xv[c] = t
        return total + t * t

    spread_t[...] = lax.fori_loop(0, cols, truth_column, jnp.zeros((nvars, lanes), jnp.float32))

    def sums(i):
        copies[i].wait()
        v0 = chunk_vars[i]

        def one(v, carry):
            sq = off = pr = sp = None
            for c in range(cols):
                n_ = xn[c, pl.ds(v0 + v, 1), :]
                t_ = xv[c, pl.ds(v0 + v, 1), :]
                f = kf[c:c + 1, :] * (xp[i, v, c] - n_)
                e = f - t_
                if sq is None:
                    sq, off, pr, sp = e * e, e, f * t_, f * f
                else:
                    sq, off, pr, sp = sq + e * e, off + e, pr + f * t_, sp + f * f
            part[i, v] = sq
            part[i, vp + v] = off
            part[i, 2 * vp + v] = pr
            part[i, 3 * vp + v] = sp
            return carry

        lax.fori_loop(0, vp, one, 0)
        for v in range(vp):
            part[i, 4 * vp + v // 4, v % 4:v % 4 + 1, :] = spread_t[pl.ds(v0 + v, 1), :]

    def remote(src, dst, s, r, device):
        return pltpu.make_async_remote_copy(src_ref=src, dst_ref=dst, send_sem=s, recv_sem=r, device_id=device, device_id_type=MESH)

    partner = (band, a * pair + ob)
    sent = []
    phase_one = {}
    greeted = False
    for i, (k, away) in enumerate(order):
        sums(i)
        if not greeted:
            pl.semaphore_wait(barrier, n_lon - 1 + n_lat - 1)
            greeted = True
        if away:
            c = remote(part.at[i], one_in.at[k], one_s.at[k], one_r.at[k], partner)
            c.start()
            phase_one[k] = c
            sent.append(c)
    phase_two = {}
    base = len(order) - outer
    for q, k in enumerate(steps):
        local = part[base + q]
        if pair == 2:
            phase_one[k].wait_recv()
            local = local + one_in[k]
        if k:
            two_out[k] = local
            c = remote(two_out.at[k], two_in.at[k], two_s.at[k], two_r.at[k], (band, other(k) * pair + b))
            c.start()
            phase_two[k] = c
            sent.append(c)
        else:
            tot[...] = local
    for k in range(1, outer):
        phase_two[k].wait_recv()
    total = tot[...]
    for k in range(1, outer):
        total = total + two_in[k]
    tot[...] = total

    points = 1.0 / float(cols * n_lon)
    for v in range(vp):
        sq, off, pr, sp = [tot[s * vp + v] for s in range(4)]
        tr = jnp.broadcast_to(tot[4 * vp + v // 4, v % 4:v % 4 + 1, :], (leads, lanes))
        for s, x in enumerate((sq, off, pr, sp, tr)):
            flat[s, pl.ds(v, leads, stride=vp), :] = x
    g_out[...] = jnp.zeros_like(g_out)
    for s in range(5):
        d = lax.dot_general(weight, flat[s], (((1,), (1,)), ((), ())), precision=lax.Precision.HIGHEST,
                            preferred_element_type=jnp.float32)
        g_out[s:s + 1, 0:lv] = d[0:1, :]
    lat_copies = []
    for k in range(1, n_lat):
        c = remote(g_out, g_in.at[k], lat_s.at[k], lat_r.at[k], (lax.rem(band + k, n_lat), me))
        c.start()
        lat_copies.append(c)
        sent.append(c)

    for v in range(vp):
        sq, off, pr, sp = [tot[s * vp + v] * points for s in range(4)]
        tr = jnp.broadcast_to(tot[4 * vp + v // 4, v % 4:v % 4 + 1, :], (leads, lanes)) * points
        fin[me, v] = sq
        fin[me, vp + v] = off
        fin[me, 2 * vp + v] = pr / jnp.sqrt(jnp.maximum(sp, FLOOR) * jnp.maximum(tr, FLOOR))
    gather_z, gather_y = {}, {}
    if pair == 2:
        c = remote(fin.at[me], fin.at[me], agy_s.at[0], agy_r.at[0], partner)
        c.start()
        gather_y[0] = c
        sent.append(c)
    for k in range(1, outer):
        c = remote(fin.at[me], fin.at[me], agz_s.at[k], agz_r.at[k], (band, other(k) * pair + b))
        c.start()
        gather_z[k] = c
        sent.append(c)

    for c in lat_copies:
        c.wait_recv()
    gs = g_out[...]
    for k in range(1, n_lat):
        gs = gs + g_in[k]
    gs = gs / float(total_rows * cols * n_lon)
    g_mine[...] = gs
    g_all[me, 0:1, :] = jnp.sqrt(jnp.maximum(g_mine[0:1, :], FLOOR))
    g_all[me, 1:2, :] = g_mine[1:2, :]
    g_all[me, 2:3, :] = g_mine[2:3, :] / jnp.sqrt(
        jnp.maximum(g_mine[3:4, :], FLOOR) * jnp.maximum(g_mine[4:5, :], FLOOR))
    g_all[me, 3:8, :] = jnp.zeros((5, g_all.shape[2]), jnp.float32)
    lon_copies = []
    for k in range(1, n_lon):
        c = remote(g_all.at[me], g_all.at[me], lon_s.at[k], lon_r.at[k], (band, lax.rem(me + k, n_lon)))
        c.start()
        lon_copies.append(c)
        sent.append(c)

    for k in sorted(range(1, outer), key=lambda k: min(k, outer - k)):
        gather_z[k].wait_recv()
        if pair == 2:
            source = fin.at[lax.rem(a - k + outer, outer) * pair + b]
            c = remote(source, source, agy_s.at[k], agy_r.at[k], partner)
            c.start()
            gather_y[k] = c
            sent.append(c)
    for c in lon_copies:
        c.wait_recv()
    for d in range(n_lon):
        for l in range(leads):
            g_tmp[l, 0:3, starts[d]:starts[d] + vp] = g_all[d, 0:3, l * vp:(l + 1) * vp]
    for l in range(leads):
        for m, out in enumerate((g_rmse, g_off, g_skill)):
            out[l:l + 1, :] = g_tmp[l, m:m + 1, 0:nvars]
    for k in gather_y:
        gather_y[k].wait_recv()
    for d in range(n_lon):
        for m, out in enumerate((o_sq, o_off, o_skill)):
            out[starts[d]:starts[d] + vp] = fin[d, m * vp:(m + 1) * vp]
    for c in sent:
        c.wait_send()


def writer(a, b, c, d, e, f, *rest):
    sem = rest[6]
    copies = [pltpu.make_async_copy(x, y, sem.at[i]) for i, (x, y) in enumerate(zip((a, b, c, d, e, f), rest[:6]))]
    for c in copies:
        c.start()
    for c in copies:
        c.wait()


def local(n_lat, n_lon, pred, ver, norm, flag, par):
    leads, nvars, cols, lanes = pred.shape
    vp = -(-nvars // n_lon)
    outer = n_lon // 2 if n_lon % 2 == 0 else n_lon
    blocks = 4 * vp + -(-vp // 4)
    glanes = -(-leads * vp // 128) * 128
    f32 = jnp.float32
    dma = pltpu.SemaphoreType.DMA
    vmem = pl.BlockSpec(memory_space=pltpu.VMEM)
    hbm = pl.BlockSpec(memory_space=pl.ANY)
    zonal = jax.ShapeDtypeStruct((nvars, leads, lanes), f32)
    whole = jax.ShapeDtypeStruct((leads, nvars), f32)
    out = pl.pallas_call(
        functools.partial(kernel, n_lat, n_lon, vp),
        out_shape=(pltpu.VMEM((nvars, leads, lanes), f32),) * 3 + (pltpu.VMEM((leads, nvars), f32),) * 3,
        in_specs=[pl.BlockSpec(memory_space=pltpu.SMEM)] + [hbm] * 4,
        out_specs=(vmem,) * 6,
        scratch_shapes=[
            pltpu.VMEM((n_lon, vp, cols, leads, lanes), f32),
            pltpu.VMEM((cols, nvars, lanes), f32),
            pltpu.VMEM((cols, nvars, lanes), f32),
            pltpu.VMEM((cols, lanes), jnp.int32),
            pltpu.VMEM((cols, lanes), f32),
            pltpu.VMEM((nvars, lanes), f32),
            pltpu.VMEM((n_lon, blocks, 4, lanes), f32),
            pltpu.VMEM((outer, blocks, 4, lanes), f32),
            pltpu.VMEM((outer, blocks, 4, lanes), f32),
            pltpu.VMEM((outer, blocks, 4, lanes), f32),
            pltpu.VMEM((blocks, 4, lanes), f32),
            pltpu.VMEM((5, leads * vp, lanes), f32),
            pltpu.VMEM((n_lon, 3 * vp, leads, lanes), f32),
            pltpu.VMEM((8, glanes), f32),
            pltpu.VMEM((n_lat, 8, glanes), f32),
            pltpu.VMEM((8, glanes), f32),
            pltpu.VMEM((n_lon, 8, glanes), f32),
            pltpu.VMEM((leads, 8, 128 * (-(-nvars // 128))), f32),
            dma((3,)), dma((n_lon,)),
            dma((outer,)), dma((outer,)), dma((outer,)), dma((outer,)),
            dma((outer,)), dma((outer,)), dma((outer,)), dma((outer,)),
            dma((n_lat,)), dma((n_lat,)), dma((n_lon,)), dma((n_lon,)),
        ],
        compiler_params=pltpu.CompilerParams(collective_id=0, has_side_effects=True, vmem_limit_bytes=LIMIT),
    )(par, jnp.transpose(pred, (1, 2, 0, 3)), jnp.transpose(ver, (1, 0, 2)), jnp.transpose(norm, (1, 0, 2)), flag)
    out = pl.pallas_call(
        writer,
        out_shape=(zonal,) * 3 + (whole,) * 3,
        in_specs=[vmem] * 6,
        out_specs=(hbm,) * 6,
        scratch_shapes=[dma((6,))],
        compiler_params=pltpu.CompilerParams(vmem_limit_bytes=4 << 20),
    )(*out)
    return tuple(jnp.transpose(x, (1, 0, 2)) for x in out[:3]) + tuple(out[3:])


def solution(mesh):
    n_lat, n_lon = mesh.shape["lat"], mesh.shape["lon"]
    in_specs = (
        P(None, None, "lon", "lat"),
        P(None, "lon", "lat"),
        P(None, "lon", "lat"),
        P("lon", "lat"),
        P(),
    )
    out_specs = (P(None, None, "lat"), P(None, None, "lat"), P(None, None, "lat"), P(), P(), P())
    return jax.shard_map(functools.partial(local, n_lat, n_lon), mesh=mesh, in_specs=in_specs, out_specs=out_specs,
                         check_vma=False)
```

```python
import functools
import math

import jax
import jax.numpy as jnp
from jax import lax
from jax.experimental import pallas as pl
from jax.experimental.pallas import tpu as pltpu
from jax.sharding import PartitionSpec as P

MEAN_ROWS = 90
FLOOR = 0.1
MESH = pl.DeviceIdType.MESH
LIMIT = 58 << 20


def cosine(y):
    y2 = y * y
    terms = [(-1) ** k / math.factorial(2 * k) for k in range(9)]
    total = jnp.full_like(y, terms[-1])
    for term in terms[-2::-1]:
        total = total * y2 + term
    return total


def split(n_lon, vp):
    pair = 2 if n_lon % 2 == 0 else 1
    groups = max(g for g in (1, 2, 3) if vp % g == 0)
    return pair, n_lon // pair, groups


def kernel(n_lat, n_lon, vp, par, pred, ver, norm, flag, zon, g_rmse, g_off, g_skill,
           xp, xv, xn, xf, kf, spread_t, part, one_in, two_out, two_in, flat, g_out, g_in, g_mine,
           in_sem, pred_sem, out_s, one_r, two_r, agz_r, agy_r, g_r):
    nvars, cols, leads, lanes = pred.shape
    pair, outer, groups = split(n_lon, vp)
    gv = vp // groups
    gb = 4 * gv - (-gv // leads)
    band = lax.axis_index("lat")
    me = lax.axis_index("lon")
    a, b = me // pair, me % pair
    ob = (pair - 1) - b
    wide = flat.shape[1] // leads
    paired = outer & (outer - 1) == 0

    def first_var(d):
        return jnp.minimum(d * vp, nvars - vp)

    def flip(k):
        other, bit = a, 1
        while bit <= k:
            if k & bit:
                other = other + bit * (1 - 2 * ((a // bit) % 2))
            bit *= 2
        return other

    def to(k):
        return flip(k) if paired else lax.rem(a + k, outer)

    def source(k):
        return flip(k) if paired else lax.rem(a - k + outer, outer)

    far = list(range(outer - 1, 0, -1))
    steps = far + [0]
    order = [(k, True) for k in steps] if pair == 2 else []
    base = len(order)
    order += [(k, False) for k in steps]
    barrier = pltpu.get_barrier_semaphore()
    for k in range(1, n_lon):
        pl.semaphore_signal(barrier, inc=1, device_id=(band, lax.rem(me + k, n_lon)), device_id_type=MESH)
    for k in range(1, n_lat):
        pl.semaphore_signal(barrier, inc=1, device_id=(lax.rem(band + k, n_lat), me), device_id_type=MESH)

    first = [
        pltpu.make_async_copy(flag, xf, in_sem.at[0]),
        pltpu.make_async_copy(norm, xn, in_sem.at[1]),
        pltpu.make_async_copy(ver, xv, in_sem.at[2]),
    ]
    for c in first:
        c.start()
    chunk_vars, copies = [], []
    for i, (k, away) in enumerate(order):
        v0 = first_var(to(k) * pair + (ob if away else b))
        chunk_vars.append(v0)
        copies.append(pltpu.make_async_copy(pred.at[pl.ds(v0, vp)], xp.at[i], pred_sem.at[i]))
    copies[0].start()

    first_row = jnp.int32(0)
    filled = jnp.int32(0)
    for i in range(n_lat):
        first_row = first_row + jnp.where(i < band, par[i], 0)
        filled = filled + jnp.where(i == band, par[i], 0)
    total_rows = MEAN_ROWS * n_lat + 1
    slot = lax.broadcasted_iota(jnp.int32, (8, lanes), 1)
    g_row = (first_row + slot).astype(jnp.float32)
    normalizer = sum(math.sin(math.pi * r / (total_rows - 1)) for r in range(total_rows))
    angle = (g_row - 0.5 * (total_rows - 1)) * (math.pi / (total_rows - 1))
    weight = jnp.where(slot < filled, cosine(angle) * (total_rows / normalizer), 0.0)
    if gv % leads:
        for i in range(n_lon):
            for g in range(groups):
                part[i, g * gb + gb - 1] = jnp.zeros((leads, lanes), jnp.float32)

    first[0].wait()
    kf[...] = jnp.where(lax.broadcasted_iota(jnp.int32, (cols, lanes), 1) < filled, xf[...].astype(jnp.float32), 0.0)
    first[1].wait()
    first[2].wait()
    for c in copies[1:]:
        c.start()

    def truth_column(c, total):
        t = kf[pl.ds(c, 1), :] * (xv[c] - xn[c])
        xv[c] = t
        return total + t * t

    spread_t[...] = lax.fori_loop(0, cols, truth_column, jnp.zeros((nvars, lanes), jnp.float32))

    def sums(i):
        copies[i].wait()
        v0 = chunk_vars[i]

        def one(v, carry):
            sq = off = pr = sp = None
            for c in range(cols):
                n_ = xn[c, pl.ds(v0 + v, 1), :]
                t_ = xv[c, pl.ds(v0 + v, 1), :]
                f = kf[c:c + 1, :] * (xp[i, v, c] - n_)
                e = f - t_
                if sq is None:
                    sq, off, pr, sp = e * e, e, f * t_, f * f
                else:
                    sq, off, pr, sp = sq + e * e, off + e, pr + f * t_, sp + f * f
            row = v * 4 + (v // gv) * (gb - 4 * gv)
            part[i, row] = sq
            part[i, row + 1] = off
            part[i, row + 2] = pr
            part[i, row + 3] = sp
            tr = jnp.broadcast_to(spread_t[pl.ds(v0 + v, 1), :], (leads, lanes))
            for s, x in enumerate((sq, off, pr, sp, tr)):
                flat[s, pl.ds(v0 + v, leads, stride=wide), :] = x
            return carry

        lax.fori_loop(0, vp, one, 0)
        for v in range(vp):
            g, r = divmod(v, gv)
            part[i, g * gb + 4 * gv + r // leads, r % leads:r % leads + 1, :] = spread_t[pl.ds(v0 + v, 1), :]

    def block(g):
        return pl.ds(g * gb, gb)

    def send(src, dst, s, r, device):
        c = pltpu.make_async_remote_copy(src_ref=src, dst_ref=dst, send_sem=s, recv_sem=r, device_id=device, device_id_type=MESH)
        c.start()
        return c

    def await_bytes(ref, s):
        pltpu.make_async_copy(ref, ref, s).wait()

    partner = (band, a * pair + ob)
    phase_one, gather_z = {}, {}

    def send_one(g, q, k):
        phase_one[g, k] = send(part.at[q, block(g)], one_in.at[k, block(g)], out_s.at[0], one_r.at[g, k], partner)

    greeted = False
    for q, k in enumerate(steps if pair == 2 else []):
        sums(q)
        if not greeted:
            pl.semaphore_wait(barrier, n_lon - 1 + n_lat - 1)
            greeted = True
        send_one(0, q, k)
    for g in range(1, groups):
        for q, k in enumerate(steps if pair == 2 else []):
            send_one(g, q, k)

    def stage_a(g):
        for q, k in enumerate(steps):
            if g == 0:
                sums(base + q)
                if base == 0 and q == 0:
                    pl.semaphore_wait(barrier, n_lon - 1 + n_lat - 1)
            local = part[base + q, block(g)]
            if pair == 2:
                phase_one[g, k].wait_recv()
                local = local + one_in[k, block(g)]
            two_out[k, block(g)] = local
            if k:
                send(two_out.at[k, block(g)], two_in.at[k, block(g)], out_s.at[1], two_r.at[g],
                                     (band, to(k) * pair + b))

    points = 1.0 / float(cols * n_lon)

    def rows_of(d, g):
        return zon.at[pl.ds(d * vp + g * gv, gv)]

    def stage_b(g):
        await_bytes(two_in.at[pl.ds(1, outer - 1), block(g)], two_r.at[g])

        def total(j):
            x = two_out[0, g * gb + j]
            for k in far:
                x = x + two_in[k, g * gb + j]
            return x

        truths = [total(4 * gv + j) for j in range(gb - 4 * gv)]
        for r in range(gv):
            sq, off, pr, sp = [total(4 * r + s) for s in range(4)]
            tr = jnp.broadcast_to(truths[r // leads][r % leads:r % leads + 1, :], (leads, lanes))
            row = me * vp + g * gv + r
            zon[row, 0] = sq * points
            zon[row, 1] = off * points
            zon[row, 2] = pr * points / jnp.sqrt(jnp.maximum(sp * points, FLOOR) * jnp.maximum(tr * points, FLOOR))
        mine = rows_of(me, g)
        for k in far:
            gather_z[g, k] = send(mine, mine, out_s.at[2], agz_r.at[g, k - 1], (band, to(k) * pair + b))
        if pair == 2:
            send(mine, mine, out_s.at[3], agy_r, partner)

    def stage_c(g):
        for k in far:
            gather_z[g, k].wait_recv()
            if pair == 2:
                block_k = rows_of(source(k) * pair + b, g)
                send(block_k, block_k, out_s.at[3], agy_r, partner)

    near = n_lat - 1 + pair - 1

    def gather(first_k, n, r, total):
        if n:
            await_bytes(g_in.at[pl.ds(first_k, n)], r)
        for k in range(first_k, first_k + n):
            total = total + g_in[k]
        return total

    def global_sums():
        for s in range(5):
            d = lax.dot_general(weight, flat[s], (((1,), (1,)), ((), ())), precision=lax.Precision.HIGHEST,
                                preferred_element_type=jnp.float32)
            g_out[0, s:s + 1, 0:leads * wide] = d[0:1, :]
        for k in range(1, n_lat):
            send(g_out.at[0], g_in.at[k - 1], out_s.at[4], g_r.at[0], (lax.rem(band + k, n_lat), me))

    def global_band():
        g_out[1] = gather(0, n_lat - 1, g_r.at[0], g_out[0])
        if pair == 2:
            send(g_out.at[1], g_in.at[n_lat - 1], out_s.at[4], g_r.at[1], partner)

    def global_pair():
        g_out[2] = gather(n_lat - 1, pair - 1, g_r.at[1], g_out[1])
        for k in far:
            send(g_out.at[2], g_in.at[near + k - 1], out_s.at[4], g_r.at[2], (band, to(k) * pair + b))

    def global_scores():
        gs = gather(near, outer - 1, g_r.at[2], g_out[2])
        g_mine[...] = gs / float(total_rows * cols * n_lon)
        mse, off, pr, sp, tr = [g_mine[s:s + 1, :] for s in range(5)]
        rmse = jnp.sqrt(jnp.maximum(mse, FLOOR))
        skill = pr / jnp.sqrt(jnp.maximum(sp, FLOOR) * jnp.maximum(tr, FLOOR))
        for l in range(leads):
            for x, out in ((rmse, g_rmse), (off, g_off), (skill, g_skill)):
                out[l:l + 1, :] = x[:, l * wide:l * wide + nvars]

    for t in range(groups + 2):
        if t < groups:
            stage_a(t)
        if t == 0:
            global_sums()
        if t == groups - 1:
            global_band()
        if 0 <= t - 1 < groups:
            stage_b(t - 1)
        if 0 <= t - 2 < groups:
            stage_c(t - 2)
        if t == groups - 1:
            global_pair()
    global_scores()
    if pair == 2:
        await_bytes(zon.at[pl.ds(0, outer * vp)], agy_r)
        await_bytes(one_in, out_s.at[0])
        await_bytes(zon.at[pl.ds(0, outer * vp)], out_s.at[3])
    await_bytes(two_in.at[pl.ds(1, outer - 1)], out_s.at[1])
    await_bytes(zon.at[pl.ds(0, (outer - 1) * vp)], out_s.at[2])
    await_bytes(g_in, out_s.at[4])


def pieces_of(nvars, n_lon, vp):
    pieces, covered = [], 0
    for d in range(n_lon):
        start = min(d * vp, nvars - vp)
        if start + vp > covered:
            n = start + vp - covered
            src = d * vp + covered - start
            if pieces and pieces[-1][0] + pieces[-1][2] == src:
                pieces[-1][2] += n
            else:
                pieces.append([src, covered, n])
            covered += n
    return pieces


def writer(n_lon, vp, zon, g_rmse, g_off, g_skill, o_sq, o_off, o_skill, o_rmse, o_moff, o_mskill, sem):
    copies = []
    for src, dst, n in pieces_of(o_sq.shape[0], n_lon, vp):
        for m, out in enumerate((o_sq, o_off, o_skill)):
            copies.append((zon.at[pl.ds(src, n), m], out.at[pl.ds(dst, n)]))
    copies += [(g_rmse, o_rmse), (g_off, o_moff), (g_skill, o_mskill)]
    copies = [pltpu.make_async_copy(x, y, sem.at[i]) for i, (x, y) in enumerate(copies)]
    for c in copies:
        c.start()
    for c in copies:
        c.wait()


def local(n_lat, n_lon, pred, ver, norm, flag, par):
    leads, nvars, cols, lanes = pred.shape
    vp = -(-nvars // n_lon)
    pair, outer, groups = split(n_lon, vp)
    blocks = groups * (4 * (vp // groups) - (-(vp // groups) // leads))
    wide = -(-nvars // 8) * 8
    glanes = -(-leads * wide // 128) * 128
    hops = n_lat - 1 + pair - 1 + outer - 1
    f32 = jnp.float32
    dma = pltpu.SemaphoreType.DMA
    vmem = pl.BlockSpec(memory_space=pltpu.VMEM)
    hbm = pl.BlockSpec(memory_space=pl.ANY)
    zonal = jax.ShapeDtypeStruct((nvars, leads, lanes), f32)
    whole = jax.ShapeDtypeStruct((leads, nvars), f32)
    inner = pl.pallas_call(
        functools.partial(kernel, n_lat, n_lon, vp),
        out_shape=(pltpu.VMEM((n_lon * vp, 3, leads, lanes), f32),) + (pltpu.VMEM((leads, nvars), f32),) * 3,
        in_specs=[pl.BlockSpec(memory_space=pltpu.SMEM)] + [hbm] * 4,
        out_specs=(vmem,) * 4,
        scratch_shapes=[
            pltpu.VMEM((n_lon, vp, cols, leads, lanes), f32),
            pltpu.VMEM((cols, nvars, lanes), f32),
            pltpu.VMEM((cols, nvars, lanes), f32),
            pltpu.VMEM((cols, lanes), jnp.int32),
            pltpu.VMEM((cols, lanes), f32),
            pltpu.VMEM((nvars, lanes), f32),
            pltpu.VMEM((n_lon, blocks, leads, lanes), f32),
            pltpu.VMEM((outer, blocks, leads, lanes), f32),
            pltpu.VMEM((outer, blocks, leads, lanes), f32),
            pltpu.VMEM((outer, blocks, leads, lanes), f32),
            pltpu.VMEM((5, leads * wide, lanes), f32),
            pltpu.VMEM((3, 5, glanes), f32),
            pltpu.VMEM((hops, 5, glanes), f32),
            pltpu.VMEM((5, glanes), f32),
            dma((3,)), dma((n_lon,)), dma((5,)),
            dma((groups, outer)), dma((groups,)), dma((groups, outer - 1)), dma, dma((3,)),
        ],
        compiler_params=pltpu.CompilerParams(collective_id=0, has_side_effects=True, vmem_limit_bytes=LIMIT),
    )(par, jnp.transpose(pred, (1, 2, 0, 3)), jnp.transpose(ver, (1, 0, 2)), jnp.transpose(norm, (1, 0, 2)), flag)
    out = pl.pallas_call(
        functools.partial(writer, n_lon, vp),
        out_shape=(zonal,) * 3 + (whole,) * 3,
        in_specs=[vmem] * 4,
        out_specs=(hbm,) * 6,
        scratch_shapes=[dma((3 * len(pieces_of(nvars, n_lon, vp)) + 3,))],
        compiler_params=pltpu.CompilerParams(vmem_limit_bytes=4 << 20),
    )(*inner)
    return tuple(jnp.transpose(x, (1, 0, 2)) for x in out[:3]) + tuple(out[3:])


def solution(mesh):
    n_lat, n_lon = mesh.shape["lat"], mesh.shape["lon"]
    in_specs = (
        P(None, None, "lon", "lat"),
        P(None, "lon", "lat"),
        P(None, "lon", "lat"),
        P("lon", "lat"),
        P(),
    )
    out_specs = (P(None, None, "lat"), P(None, None, "lat"), P(None, None, "lat"), P(), P(), P())
    return jax.shard_map(functools.partial(local, n_lat, n_lon), mesh=mesh, in_specs=in_specs, out_specs=out_specs,
                         check_vma=False)
```

```python
import functools
import math

import jax
import jax.numpy as jnp
from jax import lax
from jax.experimental import pallas as pl
from jax.experimental.pallas import tpu as pltpu
from jax.sharding import PartitionSpec as P

MEAN_ROWS = 90
FLOOR = 0.1
MESH = pl.DeviceIdType.MESH
LIMIT = 58 << 20


def cosine(y):
    y2 = y * y
    terms = [(-1) ** k / math.factorial(2 * k) for k in range(9)]
    total = jnp.full_like(y, terms[-1])
    for term in terms[-2::-1]:
        total = total * y2 + term
    return total


def split(n_lon, vp):
    pair = 2 if n_lon % 2 == 0 else 1
    groups = max(g for g in (1, 2, 3) if vp % g == 0)
    return pair, n_lon // pair, groups


def kernel(n_lat, n_lon, vp, par, pred, ver, norm, flag, zon, g_rmse, g_off, g_skill,
           xp, xt, xf, kf, spread_t, part, one_in, two_out, two_in, flat, g_in, g_mine,
           in_sem, pred_sem, out_s, one_r, two_r, agz_r, agy_r, g_r):
    nvars, cols, leads, lanes = pred.shape
    pair, outer, groups = split(n_lon, vp)
    gv = vp // groups
    gb = 4 * gv - (-gv // leads)
    band = lax.axis_index("lat")
    me = lax.axis_index("lon")
    a, b = me // pair, me % pair
    ob = (pair - 1) - b
    wide = flat.shape[1] // leads
    paired = outer & (outer - 1) == 0

    def first_var(d):
        return jnp.minimum(d * vp, nvars - vp)

    def flip(k):
        other, bit = a, 1
        while bit <= k:
            if k & bit:
                other = other + bit * (1 - 2 * ((a // bit) % 2))
            bit *= 2
        return other

    def to(k):
        return flip(k) if paired else lax.rem(a + k, outer)

    def source(k):
        return flip(k) if paired else lax.rem(a - k + outer, outer)

    far = list(range(outer - 1, 0, -1))
    steps = far + [0]
    order = [(k, True) for k in steps] if pair == 2 else []
    base = len(order)
    order += [(k, False) for k in steps]
    pieces = 3 if cols % 3 == 0 else 1
    span = cols // pieces
    xn, xv = xt.at[0], xt.at[1]
    flags = pltpu.make_async_copy(flag, xf, in_sem.at[pieces])
    flags.start()
    for p in range(pieces):
        here = pl.ds(p * span, span)
        pltpu.make_async_copy(norm.at[here], xt.at[0, here], in_sem.at[p]).start()
        pltpu.make_async_copy(ver.at[here], xt.at[1, here], in_sem.at[p]).start()
    chunk_vars, copies = [], []
    for i, (k, away) in enumerate(order):
        v0 = first_var(to(k) * pair + (ob if away else b))
        chunk_vars.append(v0)
        copies.append(pltpu.make_async_copy(pred.at[pl.ds(v0, vp)], xp.at[i], pred_sem.at[i]))
    copies[0].start()

    barrier = pltpu.get_barrier_semaphore()
    for k in range(1, n_lon):
        pl.semaphore_signal(barrier, inc=1, device_id=(band, lax.rem(me + k, n_lon)), device_id_type=MESH)
    for k in range(1, n_lat):
        for there in ([me, a * pair + ob] if pair == 2 else [me]):
            pl.semaphore_signal(barrier, inc=1, device_id=(lax.rem(band + k, n_lat), there), device_id_type=MESH)

    first_row = jnp.int32(0)
    filled = jnp.int32(0)
    for i in range(n_lat):
        first_row = first_row + jnp.where(i < band, par[i], 0)
        filled = filled + jnp.where(i == band, par[i], 0)
    if gv % leads:
        for i in range(n_lon):
            for g in range(groups):
                part[i, g * gb + gb - 1] = jnp.zeros((leads, lanes), jnp.float32)

    flags.wait()
    kf[...] = jnp.where(lax.broadcasted_iota(jnp.int32, (cols, lanes), 1) < filled, xf[...].astype(jnp.float32), 0.0)

    def truth_column(c, total):
        t = kf[pl.ds(c, 1), :] * (xv[c] - xn[c])
        xv[c] = t
        return total + t * t

    truth_total = jnp.zeros((nvars, lanes), jnp.float32)
    for p in range(pieces):
        here = xt.at[:, pl.ds(p * span, span)]
        pltpu.make_async_copy(here, here, in_sem.at[p]).wait()
        if p == 0:
            for c in copies[1:]:
                c.start()
        truth_total = lax.fori_loop(p * span, (p + 1) * span, truth_column, truth_total, unroll=5 if span % 5 == 0 else 1)
    spread_t[...] = truth_total

    def sums(i, g):
        if g == 0:
            copies[i].wait()
        v0 = chunk_vars[i]

        def one(r, carry):
            v = g * gv + r
            sq = off = pr = sp = None
            for c in range(cols):
                n_ = xn[c, pl.ds(v0 + v, 1), :]
                t_ = xv[c, pl.ds(v0 + v, 1), :]
                f = kf[c:c + 1, :] * (xp[i, v, c] - n_)
                e = f - t_
                if sq is None:
                    sq, off, pr, sp = e * e, e, f * t_, f * f
                else:
                    sq, off, pr, sp = sq + e * e, off + e, pr + f * t_, sp + f * f
            row = g * gb + r * 4
            part[i, row] = sq
            part[i, row + 1] = off
            part[i, row + 2] = pr
            part[i, row + 3] = sp
            tr = jnp.broadcast_to(spread_t[pl.ds(v0 + v, 1), :], (leads, lanes))
            for s, x in enumerate((sq, off, pr, sp, tr)):
                flat[s, pl.ds(v0 + v, leads, stride=wide), :] = x
            return carry

        lax.fori_loop(0, gv, one, 0)
        for r in range(gv):
            part[i, g * gb + 4 * gv + r // leads, r % leads:r % leads + 1, :] = spread_t[pl.ds(v0 + g * gv + r, 1), :]

    def block(g):
        return pl.ds(g * gb, gb)

    def send(src, dst, s, r, device):
        c = pltpu.make_async_remote_copy(src_ref=src, dst_ref=dst, send_sem=s, recv_sem=r, device_id=device, device_id_type=MESH)
        c.start()
        return c

    def await_bytes(ref, s):
        pltpu.make_async_copy(ref, ref, s).wait()

    partner = (band, a * pair + ob)
    phase_one, gather_z = {}, {}

    def send_one(g, q, k):
        phase_one[g, k] = send(part.at[q, block(g)], one_in.at[k, block(g)], out_s.at[0], one_r.at[g, k], partner)

    greeted = []

    def greet():
        if not greeted:
            pl.semaphore_wait(barrier, n_lon - 1 + (n_lat - 1) * pair)
            greeted.append(True)

    def away(g):
        for q, k in enumerate(steps if pair == 2 else []):
            sums(q, g)
            greet()
            send_one(g, q, k)

    def stage_a(g, q):
        k = steps[q]
        greet()
        local = part[base + q, block(g)]
        if pair == 2:
            phase_one[g, k].wait_recv()
            local = local + one_in[k, block(g)]
        two_out[k, block(g)] = local
        if k:
            send(two_out.at[k, block(g)], two_in.at[k, block(g)], out_s.at[1], two_r.at[g], (band, to(k) * pair + b))

    points = 1.0 / float(cols * n_lon)

    def rows_of(d, g):
        return zon.at[pl.ds(d * vp + g * gv, gv)]

    def stage_b(g):
        await_bytes(two_in.at[pl.ds(1, outer - 1), block(g)], two_r.at[g])

        def total(j):
            x = two_out[0, g * gb + j]
            for k in far:
                x = x + two_in[k, g * gb + j]
            return x

        truths = [total(4 * gv + j) for j in range(gb - 4 * gv)]
        for r in range(gv):
            sq, off, pr, sp = [total(4 * r + s) for s in range(4)]
            tr = jnp.broadcast_to(truths[r // leads][r % leads:r % leads + 1, :], (leads, lanes))
            row = me * vp + g * gv + r
            zon[row, 0] = sq * points
            zon[row, 1] = off * points
            zon[row, 2] = pr * points / jnp.sqrt(jnp.maximum(sp * points, FLOOR) * jnp.maximum(tr * points, FLOOR))
        mine = rows_of(me, g)
        for k in far:
            gather_z[g, k] = send(mine, mine, out_s.at[2], agz_r.at[g, k - 1], (band, to(k) * pair + b))
        if pair == 2:
            send(mine, mine, out_s.at[3], agy_r, partner)

    def stage_c(g):
        for k in far:
            gather_z[g, k].wait_recv()
            if pair == 2:
                block_k = rows_of(source(k) * pair + b, g)
                send(block_k, block_k, out_s.at[3], agy_r, partner)

    near = n_lat * pair

    def global_sums():
        total_rows = MEAN_ROWS * n_lat + 1
        slot = lax.broadcasted_iota(jnp.int32, (8, lanes), 1)
        g_row = (first_row + slot).astype(jnp.float32)
        normalizer = sum(math.sin(math.pi * r / (total_rows - 1)) for r in range(total_rows))
        angle = (g_row - 0.5 * (total_rows - 1)) * (math.pi / (total_rows - 1))
        weight = jnp.where(slot < filled, cosine(angle) * (total_rows / normalizer), 0.0)
        for s in range(5):
            d = lax.dot_general(weight, flat[s], (((1,), (1,)), ((), ())), precision=lax.Precision.HIGHEST,
                                preferred_element_type=jnp.float32)
            g_in[band * pair + b, s:s + 1, 0:leads * wide] = d[0:1, :]
        mine = g_in.at[band * pair + b]
        for k in range(1, near):
            device = (lax.rem(band + k % n_lat, n_lat), me if k < n_lat else a * pair + ob)
            send(mine, mine, out_s.at[4], g_r.at[0], device)

    def global_near():
        await_bytes(g_in.at[pl.ds(0, near - 1)], g_r.at[0])
        total = g_in[0]
        for k in range(1, near):
            total = total + g_in[k]
        mine = g_in.at[near + a]
        mine[...] = total
        for k in far:
            send(mine, mine, out_s.at[4], g_r.at[1], (band, to(k) * pair + b))

    def global_scores():
        await_bytes(g_in.at[pl.ds(near, outer - 1)], g_r.at[1])
        total = g_in[near]
        for k in range(1, outer):
            total = total + g_in[near + k]
        g_mine[...] = total / float((MEAN_ROWS * n_lat + 1) * cols * n_lon)
        mse, off, pr, sp, tr = [g_mine[s:s + 1, :] for s in range(5)]
        rmse = jnp.sqrt(jnp.maximum(mse, FLOOR))
        skill = pr / jnp.sqrt(jnp.maximum(sp, FLOOR) * jnp.maximum(tr, FLOOR))
        for l in range(leads):
            for x, out in ((rmse, g_rmse), (off, g_off), (skill, g_skill)):
                out[l:l + 1, :] = x[:, l * wide:l * wide + nvars]

    away(0)
    for q in range(outer):
        sums(base + q, 0)
    for g in range(1, groups):
        away(g)
        for q in range(outer):
            stage_a(g - 1, q)
            sums(base + q, g)
    global_sums()
    for q in range(outer):
        stage_a(groups - 1, q)
    for g in range(groups):
        stage_b(g)
    global_near()
    for g in range(groups):
        stage_c(g)
    global_scores()
    if pair == 2:
        await_bytes(zon.at[pl.ds(0, outer * vp)], agy_r)
        await_bytes(one_in, out_s.at[0])
        await_bytes(zon.at[pl.ds(0, outer * vp)], out_s.at[3])
    await_bytes(two_in.at[pl.ds(1, outer - 1)], out_s.at[1])
    await_bytes(zon.at[pl.ds(0, (outer - 1) * vp)], out_s.at[2])
    await_bytes(g_in.at[pl.ds(0, near + outer - 2)], out_s.at[4])


def pieces_of(nvars, n_lon, vp):
    pieces, covered = [], 0
    for d in range(n_lon):
        start = min(d * vp, nvars - vp)
        if start + vp > covered:
            n = start + vp - covered
            src = d * vp + covered - start
            if pieces and pieces[-1][0] + pieces[-1][2] == src:
                pieces[-1][2] += n
            else:
                pieces.append([src, covered, n])
            covered += n
    return pieces


def writer(n_lon, vp, zon, g_rmse, g_off, g_skill, o_sq, o_off, o_skill, o_rmse, o_moff, o_mskill, sem):
    copies = []
    for src, dst, n in pieces_of(o_sq.shape[0], n_lon, vp):
        for m, out in enumerate((o_sq, o_off, o_skill)):
            copies.append((zon.at[pl.ds(src, n), m], out.at[pl.ds(dst, n)]))
    copies += [(g_rmse, o_rmse), (g_off, o_moff), (g_skill, o_mskill)]
    copies = [pltpu.make_async_copy(x, y, sem.at[i]) for i, (x, y) in enumerate(copies)]
    for c in copies:
        c.start()
    for c in copies:
        c.wait()


def local(n_lat, n_lon, pred, ver, norm, flag, par):
    leads, nvars, cols, lanes = pred.shape
    vp = -(-nvars // n_lon)
    pair, outer, groups = split(n_lon, vp)
    blocks = groups * (4 * (vp // groups) - (-(vp // groups) // leads))
    wide = -(-nvars // 8) * 8
    glanes = -(-leads * wide // 128) * 128
    hops = n_lat * pair + outer
    f32 = jnp.float32
    dma = pltpu.SemaphoreType.DMA
    vmem = pl.BlockSpec(memory_space=pltpu.VMEM)
    hbm = pl.BlockSpec(memory_space=pl.ANY)
    zonal = jax.ShapeDtypeStruct((nvars, leads, lanes), f32)
    whole = jax.ShapeDtypeStruct((leads, nvars), f32)
    inner = pl.pallas_call(
        functools.partial(kernel, n_lat, n_lon, vp),
        out_shape=(pltpu.VMEM((n_lon * vp, 3, leads, lanes), f32),) + (pltpu.VMEM((leads, nvars), f32),) * 3,
        in_specs=[pl.BlockSpec(memory_space=pltpu.SMEM)] + [hbm] * 4,
        out_specs=(vmem,) * 4,
        scratch_shapes=[
            pltpu.VMEM((n_lon, vp, cols, leads, lanes), f32),
            pltpu.VMEM((2, cols, nvars, lanes), f32),
            pltpu.VMEM((cols, lanes), jnp.int32),
            pltpu.VMEM((cols, lanes), f32),
            pltpu.VMEM((nvars, lanes), f32),
            pltpu.VMEM((n_lon, blocks, leads, lanes), f32),
            pltpu.VMEM((outer, blocks, leads, lanes), f32),
            pltpu.VMEM((outer, blocks, leads, lanes), f32),
            pltpu.VMEM((outer, blocks, leads, lanes), f32),
            pltpu.VMEM((5, leads * wide, lanes), f32),
            pltpu.VMEM((hops, 5, glanes), f32),
            pltpu.VMEM((5, glanes), f32),
            dma((4,)), dma((n_lon,)), dma((5,)),
            dma((groups, outer)), dma((groups,)), dma((groups, outer - 1)), dma, dma((2,)),
        ],
        compiler_params=pltpu.CompilerParams(collective_id=0, has_side_effects=True, vmem_limit_bytes=LIMIT),
    )(par, jnp.transpose(pred, (1, 2, 0, 3)), jnp.transpose(ver, (1, 0, 2)), jnp.transpose(norm, (1, 0, 2)), flag)
    out = pl.pallas_call(
        functools.partial(writer, n_lon, vp),
        out_shape=(zonal,) * 3 + (whole,) * 3,
        in_specs=[vmem] * 4,
        out_specs=(hbm,) * 6,
        scratch_shapes=[dma((3 * len(pieces_of(nvars, n_lon, vp)) + 3,))],
        compiler_params=pltpu.CompilerParams(vmem_limit_bytes=4 << 20),
    )(*inner)
    return tuple(jnp.transpose(x, (1, 0, 2)) for x in out[:3]) + tuple(out[3:])


def solution(mesh):
    n_lat, n_lon = mesh.shape["lat"], mesh.shape["lon"]
    in_specs = (
        P(None, None, "lon", "lat"),
        P(None, "lon", "lat"),
        P(None, "lon", "lat"),
        P("lon", "lat"),
        P(),
    )
    out_specs = (P(None, None, "lat"), P(None, None, "lat"), P(None, None, "lat"), P(), P(), P())
    return jax.shard_map(functools.partial(local, n_lat, n_lon), mesh=mesh, in_specs=in_specs, out_specs=out_specs,
                         check_vma=False)
```

```python
import functools
import math

import jax
import jax.numpy as jnp
from jax import lax
from jax.experimental import pallas as pl
from jax.experimental.pallas import tpu as pltpu
from jax.sharding import PartitionSpec as P

MEAN_ROWS = 90
FLOOR = 0.1
MESH = pl.DeviceIdType.MESH
LIMIT = 58 << 20


def cosine(y):
    y2 = y * y
    terms = [(-1) ** k / math.factorial(2 * k) for k in range(9)]
    total = jnp.full_like(y, terms[-1])
    for term in terms[-2::-1]:
        total = total * y2 + term
    return total


def split(n_lon):
    pair = 2 if n_lon % 2 == 0 else 1
    return pair, n_lon // pair


def plan(vp):
    if vp > 4:
        return [vp // 3, vp - vp // 3 - 2, 2]
    return [1] * vp


def rows_in(sizes, leads):
    return [4 * w - (-w // leads) for w in sizes]


def kernel(n_lat, n_lon, vp, par, pred, ver, norm, flag, zon, g_rmse, g_off, g_skill,
           xp, xt, xf, kf, spread_t, part, one_in, two_out, two_in, flat, g_in, g_mine,
           in_sem, pred_sem, out_s, one_r, two_r, agz_r, agy_r, g_r):
    nvars, cols, leads, lanes = pred.shape
    pair, outer = split(n_lon)
    sizes = plan(vp)
    groups = len(sizes)
    off = [sum(sizes[:g]) for g in range(groups)]
    gbs = rows_in(sizes, leads)
    row_of = [sum(gbs[:g]) for g in range(groups)]
    band = lax.axis_index("lat")
    me = lax.axis_index("lon")
    a, b = me // pair, me % pair
    ob = (pair - 1) - b
    wide = flat.shape[1] // leads
    paired = outer & (outer - 1) == 0

    def first_var(d):
        return jnp.minimum(d * vp, nvars - vp)

    def flip(k):
        other, bit = a, 1
        while bit <= k:
            if k & bit:
                other = other + bit * (1 - 2 * ((a // bit) % 2))
            bit *= 2
        return other

    def to(k):
        return flip(k) if paired else lax.rem(a + k, outer)

    def source(k):
        return flip(k) if paired else lax.rem(a - k + outer, outer)

    far = list(range(outer - 1, 0, -1))
    steps = far + [0]
    order = [(k, True) for k in steps] if pair == 2 else []
    base = len(order)
    order += [(k, False) for k in steps]
    pieces = 3 if cols % 3 == 0 else 1
    span = cols // pieces
    xn, xv = xt.at[0], xt.at[1]
    flags = pltpu.make_async_copy(flag, xf, in_sem.at[pieces])
    flags.start()
    for p in range(pieces):
        here = pl.ds(p * span, span)
        pltpu.make_async_copy(norm.at[here], xt.at[0, here], in_sem.at[p]).start()
        pltpu.make_async_copy(ver.at[here], xt.at[1, here], in_sem.at[p]).start()
    chunk_vars, copies = [], []
    for i, (k, away) in enumerate(order):
        v0 = first_var(to(k) * pair + (ob if away else b))
        chunk_vars.append(v0)
        copies.append(pltpu.make_async_copy(pred.at[pl.ds(v0, vp)], xp.at[i], pred_sem.at[i]))
    copies[0].start()

    barrier = pltpu.get_barrier_semaphore()
    for k in range(1, n_lon):
        pl.semaphore_signal(barrier, inc=1, device_id=(band, lax.rem(me + k, n_lon)), device_id_type=MESH)
    for k in range(1, n_lat):
        for there in ([me, a * pair + ob] if pair == 2 else [me]):
            pl.semaphore_signal(barrier, inc=1, device_id=(lax.rem(band + k, n_lat), there), device_id_type=MESH)

    first_row = jnp.int32(0)
    filled = jnp.int32(0)
    for i in range(n_lat):
        first_row = first_row + jnp.where(i < band, par[i], 0)
        filled = filled + jnp.where(i == band, par[i], 0)
    for g in range(groups):
        if sizes[g] % leads:
            for i in range(n_lon):
                part[i, row_of[g] + gbs[g] - 1] = jnp.zeros((leads, lanes), jnp.float32)

    flags.wait()
    kf[...] = jnp.where(lax.broadcasted_iota(jnp.int32, (cols, lanes), 1) < filled, xf[...].astype(jnp.float32), 0.0)

    def truth_column(c, total):
        t = kf[pl.ds(c, 1), :] * (xv[c] - xn[c])
        xv[c] = t
        return total + t * t

    truth_total = jnp.zeros((nvars, lanes), jnp.float32)
    for p in range(pieces):
        here = xt.at[:, pl.ds(p * span, span)]
        pltpu.make_async_copy(here, here, in_sem.at[p]).wait()
        if p == 0:
            for c in copies[1:]:
                c.start()
        truth_total = lax.fori_loop(p * span, (p + 1) * span, truth_column, truth_total, unroll=5 if span % 5 == 0 else 1)
    spread_t[...] = truth_total

    landed = []

    def sums(i, g):
        if i not in landed:
            copies[i].wait()
            landed.append(i)
        v0 = chunk_vars[i]

        def one(r, carry):
            v = off[g] + r
            sq = off_ = pr = sp = None
            for c in range(cols):
                n_ = xn[c, pl.ds(v0 + v, 1), :]
                t_ = xv[c, pl.ds(v0 + v, 1), :]
                f = kf[c:c + 1, :] * (xp[i, v, c] - n_)
                e = f - t_
                if sq is None:
                    sq, off_, pr, sp = e * e, e, f * t_, f * f
                else:
                    sq, off_, pr, sp = sq + e * e, off_ + e, pr + f * t_, sp + f * f
            row = row_of[g] + r * 4
            part[i, row] = sq
            part[i, row + 1] = off_
            part[i, row + 2] = pr
            part[i, row + 3] = sp
            tr = jnp.broadcast_to(spread_t[pl.ds(v0 + v, 1), :], (leads, lanes))
            for s, x in enumerate((sq, off_, pr, sp, tr)):
                flat[s, pl.ds(v0 + v, leads, stride=wide), :] = x
            return carry

        lax.fori_loop(0, sizes[g], one, 0)
        for r in range(sizes[g]):
            part[i, row_of[g] + 4 * sizes[g] + r // leads, r % leads:r % leads + 1, :] = spread_t[pl.ds(v0 + off[g] + r, 1), :]

    def block(g):
        return pl.ds(row_of[g], gbs[g])

    def send(src, dst, s, r, device):
        c = pltpu.make_async_remote_copy(src_ref=src, dst_ref=dst, send_sem=s, recv_sem=r, device_id=device, device_id_type=MESH)
        c.start()
        return c

    def await_bytes(ref, s):
        pltpu.make_async_copy(ref, ref, s).wait()

    partner = (band, a * pair + ob)
    phase_one, gather_z = {}, {}

    def send_one(g, q, k):
        phase_one[g, k] = send(part.at[q, block(g)], one_in.at[k, block(g)], out_s.at[0], one_r.at[g, k], partner)

    greeted = []

    def greet():
        if not greeted:
            pl.semaphore_wait(barrier, n_lon - 1 + (n_lat - 1) * pair)
            greeted.append(True)

    def away(g, q):
        if pair == 2:
            sums(q, g)
            greet()
            send_one(g, q, steps[q])

    def stage_a(g, q):
        k = steps[q]
        greet()
        local = part[base + q, block(g)]
        if pair == 2:
            phase_one[g, k].wait_recv()
            local = local + one_in[k, block(g)]
        two_out[k, block(g)] = local
        if k:
            send(two_out.at[k, block(g)], two_in.at[k, block(g)], out_s.at[1], two_r.at[g], (band, to(k) * pair + b))

    points = 1.0 / float(cols * n_lon)

    def rows_of(d, g):
        return zon.at[pl.ds(d * vp + off[g], sizes[g])]

    def straight(g):
        return pair == 2 and g == groups - 1

    def stage_b(g):
        gv = sizes[g]
        await_bytes(two_in.at[pl.ds(1, outer - 1), block(g)], two_r.at[g])

        def total(j):
            x = two_out[0, row_of[g] + j]
            for k in far:
                x = x + two_in[k, row_of[g] + j]
            return x

        truths = [total(4 * gv + j) for j in range(gbs[g] - 4 * gv)]
        for r in range(gv):
            sq, off_, pr, sp = [total(4 * r + s) for s in range(4)]
            tr = jnp.broadcast_to(truths[r // leads][r % leads:r % leads + 1, :], (leads, lanes))
            row = me * vp + off[g] + r
            zon[row, 0] = sq * points
            zon[row, 1] = off_ * points
            zon[row, 2] = pr * points / jnp.sqrt(jnp.maximum(sp * points, FLOOR) * jnp.maximum(tr * points, FLOOR))
        mine = rows_of(me, g)
        for k in far:
            gather_z[g, k] = send(mine, mine, out_s.at[2], agz_r.at[g, k - 1], (band, to(k) * pair + b))
        if pair == 2:
            send(mine, mine, out_s.at[3], agy_r, partner)
            if straight(g):
                for k in far:
                    send(mine, mine, out_s.at[3], agy_r, (band, to(k) * pair + ob))

    def stage_c(g):
        for k in far:
            gather_z[g, k].wait_recv()
            if pair == 2 and not straight(g):
                block_k = rows_of(source(k) * pair + b, g)
                send(block_k, block_k, out_s.at[3], agy_r, partner)

    near = n_lat * pair

    def global_sums():
        total_rows = MEAN_ROWS * n_lat + 1
        slot = lax.broadcasted_iota(jnp.int32, (8, lanes), 1)
        g_row = (first_row + slot).astype(jnp.float32)
        normalizer = sum(math.sin(math.pi * r / (total_rows - 1)) for r in range(total_rows))
        angle = (g_row - 0.5 * (total_rows - 1)) * (math.pi / (total_rows - 1))
        weight = jnp.where(slot < filled, cosine(angle) * (total_rows / normalizer), 0.0)
        for s in range(5):
            d = lax.dot_general(weight, flat[s], (((1,), (1,)), ((), ())), precision=lax.Precision.HIGHEST,
                                preferred_element_type=jnp.float32)
            g_in[band * pair + b, s:s + 1, 0:leads * wide] = d[0:1, :]
        mine = g_in.at[band * pair + b]
        for k in range(1, near):
            device = (lax.rem(band + k % n_lat, n_lat), me if k < n_lat else a * pair + ob)
            send(mine, mine, out_s.at[4], g_r.at[0], device)

    def global_near():
        await_bytes(g_in.at[pl.ds(0, near - 1)], g_r.at[0])
        total = g_in[0]
        for k in range(1, near):
            total = total + g_in[k]
        mine = g_in.at[near + a]
        mine[...] = total
        for k in far:
            send(mine, mine, out_s.at[4], g_r.at[1], (band, to(k) * pair + b))

    def global_scores():
        await_bytes(g_in.at[pl.ds(near, outer - 1)], g_r.at[1])
        total = g_in[near]
        for k in range(1, outer):
            total = total + g_in[near + k]
        g_mine[...] = total / float((MEAN_ROWS * n_lat + 1) * cols * n_lon)
        mse, off_, pr, sp, tr = [g_mine[s:s + 1, :] for s in range(5)]
        rmse = jnp.sqrt(jnp.maximum(mse, FLOOR))
        skill = pr / jnp.sqrt(jnp.maximum(sp, FLOOR) * jnp.maximum(tr, FLOOR))
        for l in range(leads):
            for x, out in ((rmse, g_rmse), (off_, g_off), (skill, g_skill)):
                out[l:l + 1, :] = x[:, l * wide:l * wide + nvars]

    for q in range(outer):
        away(0, q)
    for q in range(outer):
        sums(base + q, 0)
    for g in range(1, groups):
        for q in range(outer):
            away(g, q)
            stage_a(g - 1, q)
            sums(base + q, g)
    global_sums()
    for q in range(outer):
        stage_a(groups - 1, q)
    for g in range(groups):
        if g == groups - 1:
            global_near()
        stage_b(g)
    for g in range(groups):
        stage_c(g)
    global_scores()
    if pair == 2:
        await_bytes(zon.at[pl.ds(0, outer * vp)], agy_r)
        await_bytes(one_in, out_s.at[0])
        await_bytes(zon.at[pl.ds(0, outer * vp)], out_s.at[3])
    await_bytes(two_in.at[pl.ds(1, outer - 1)], out_s.at[1])
    await_bytes(zon.at[pl.ds(0, (outer - 1) * vp)], out_s.at[2])
    await_bytes(g_in.at[pl.ds(0, near + outer - 2)], out_s.at[4])


def pieces_of(nvars, n_lon, vp):
    pieces, covered = [], 0
    for d in range(n_lon):
        start = min(d * vp, nvars - vp)
        if start + vp > covered:
            n = start + vp - covered
            src = d * vp + covered - start
            if pieces and pieces[-1][0] + pieces[-1][2] == src:
                pieces[-1][2] += n
            else:
                pieces.append([src, covered, n])
            covered += n
    return pieces


def writer(n_lon, vp, zon, g_rmse, g_off, g_skill, o_sq, o_off, o_skill, o_rmse, o_moff, o_mskill, sem):
    copies = []
    for src, dst, n in pieces_of(o_sq.shape[0], n_lon, vp):
        for m, out in enumerate((o_sq, o_off, o_skill)):
            copies.append((zon.at[pl.ds(src, n), m], out.at[pl.ds(dst, n)]))
    copies += [(g_rmse, o_rmse), (g_off, o_moff), (g_skill, o_mskill)]
    copies = [pltpu.make_async_copy(x, y, sem.at[i]) for i, (x, y) in enumerate(copies)]
    for c in copies:
        c.start()
    for c in copies:
        c.wait()


def local(n_lat, n_lon, pred, ver, norm, flag, par):
    leads, nvars, cols, lanes = pred.shape
    vp = -(-nvars // n_lon)
    pair, outer = split(n_lon)
    sizes = plan(vp)
    groups = len(sizes)
    blocks = sum(rows_in(sizes, leads))
    wide = -(-nvars // 8) * 8
    glanes = -(-leads * wide // 128) * 128
    hops = n_lat * pair + outer
    f32 = jnp.float32
    dma = pltpu.SemaphoreType.DMA
    vmem = pl.BlockSpec(memory_space=pltpu.VMEM)
    hbm = pl.BlockSpec(memory_space=pl.ANY)
    zonal = jax.ShapeDtypeStruct((nvars, leads, lanes), f32)
    whole = jax.ShapeDtypeStruct((leads, nvars), f32)
    inner = pl.pallas_call(
        functools.partial(kernel, n_lat, n_lon, vp),
        out_shape=(pltpu.VMEM((n_lon * vp, 3, leads, lanes), f32),) + (pltpu.VMEM((leads, nvars), f32),) * 3,
        in_specs=[pl.BlockSpec(memory_space=pltpu.SMEM)] + [hbm] * 4,
        out_specs=(vmem,) * 4,
        scratch_shapes=[
            pltpu.VMEM((n_lon, vp, cols, leads, lanes), f32),
            pltpu.VMEM((2, cols, nvars, lanes), f32),
            pltpu.VMEM((cols, lanes), jnp.int32),
            pltpu.VMEM((cols, lanes), f32),
            pltpu.VMEM((nvars, lanes), f32),
            pltpu.VMEM((n_lon, blocks, leads, lanes), f32),
            pltpu.VMEM((outer, blocks, leads, lanes), f32),
            pltpu.VMEM((outer, blocks, leads, lanes), f32),
            pltpu.VMEM((outer, blocks, leads, lanes), f32),
            pltpu.VMEM((5, leads * wide, lanes), f32),
            pltpu.VMEM((hops, 5, glanes), f32),
            pltpu.VMEM((5, glanes), f32),
            dma((4,)), dma((n_lon,)), dma((5,)),
            dma((groups, outer)), dma((groups,)), dma((groups, outer - 1)), dma, dma((2,)),
        ],
        compiler_params=pltpu.CompilerParams(collective_id=0, has_side_effects=True, vmem_limit_bytes=LIMIT),
    )(par, jnp.transpose(pred, (1, 2, 0, 3)), jnp.transpose(ver, (1, 0, 2)), jnp.transpose(norm, (1, 0, 2)), flag)
    out = pl.pallas_call(
        functools.partial(writer, n_lon, vp),
        out_shape=(zonal,) * 3 + (whole,) * 3,
        in_specs=[vmem] * 4,
        out_specs=(hbm,) * 6,
        scratch_shapes=[dma((3 * len(pieces_of(nvars, n_lon, vp)) + 3,))],
        compiler_params=pltpu.CompilerParams(vmem_limit_bytes=4 << 20),
    )(*inner)
    return tuple(jnp.transpose(x, (1, 0, 2)) for x in out[:3]) + tuple(out[3:])


def solution(mesh):
    n_lat, n_lon = mesh.shape["lat"], mesh.shape["lon"]
    in_specs = (
        P(None, None, "lon", "lat"),
        P(None, "lon", "lat"),
        P(None, "lon", "lat"),
        P("lon", "lat"),
        P(),
    )
    out_specs = (P(None, None, "lat"), P(None, None, "lat"), P(None, None, "lat"), P(), P(), P())
    return jax.shard_map(functools.partial(local, n_lat, n_lon), mesh=mesh, in_specs=in_specs, out_specs=out_specs,
                         check_vma=False)
```
